32 devices in a mesh: rows: 4 (over x, core), cols: 8 (over z, y).
Axes of the slice: x: 2, y: 2, z: 4, core: 2. Of those that a mesh axis runs over, the one named last changes fastest.
Arguments:
- design: bfloat16 [4096, 8192], P('rows', 'cols'), may hold values from -6 to 6
- theta: float32 [8192], P('cols'), may hold values from -0.0625 to 0.0625
- feature_scale: float32 [8192], P('cols'), may hold values from 0.05 to 2
- labels: int32 [4096], P('rows'), may hold values 0 or 1
- psi: bfloat16 [1024, 256], replicated, may hold values from -0.1875 to 0.1875
- phi: float32 [512, 256], replicated, may hold values from -0.25 to 0.25
Outputs:
- newton_step: float32 [8192], P('cols')
- sketch: float32 [256, 8192], P(None, 'cols')
The draws below stay inside these ranges and needn't reach their ends.
All inputs are finite; a program needn't handle non-finite values. No bound on the sum of `labels` on one device may be relied on, other than what follows from the above.
Results may differ from the reference program's by a relative error of at most 0.0085.
Values sent between devices are 32-bit elements; how exact they have to be, the bound alone decides.
No kernel may reach another device: no remote copies, remote signals or barrier semaphores. Data moves between devices by JAX's collectives and lax.ppermute only.
A program may use at most 128 MiB of HBM per device.

```python
import math
import jax
import jax.numpy as jnp
from jax import lax

F = 8192
S = 256
R_DEV = 1024
ITERS = 10
SAMPLES = 4096
LEVELS = 2
N_ROWS = 4


def with_ends(drawn, rng, least, high):
    longest = drawn.shape.index(max(drawn.shape))
    spots = []
    for shift in (0, 1):
        where = [jax.random.randint(jax.random.fold_in(rng, axis), (), 0, length) for axis, length in enumerate(drawn.shape)]
        where[longest] = (where[longest] + shift) % drawn.shape[longest]
        spots.append(tuple(where))
    return drawn.at[spots[0]].set(least).at[spots[1]].set(high)


def steps_of(rng, shape, shards, smallest, top_value):
    level, own = 1.0, jax.random.fold_in(rng, 6)
    for axis_at, parts in shards:
        draws = jnp.exp(jax.random.uniform(jax.random.fold_in(own, axis_at), (parts,), jnp.float32, smallest / len(shards), top_value / len(shards)))
        level = level * jnp.repeat(draws, shape[axis_at] // parts).reshape([-1 if axis == axis_at else 1 for axis in range(len(shape))])
    return level


def noise(own_key, extent, deviation, most, split=(), held_as=jnp.bfloat16):
    factor_of = steps_of(own_key, extent, split, -0.22, 0.18) if split else 1.0
    result = jax.random.normal(own_key, extent, jnp.float32) * deviation * factor_of
    return jnp.minimum(jnp.maximum(result, -most), most).astype(held_as)


def setup_inputs(seed: int = 0) -> dict:
    key_list = jax.random.split(jax.random.key(seed), 7)
    design = noise(key_list[0], (SAMPLES, F), 1.0, 6.0, ((0, 4), (1, 8)))
    theta = noise(key_list[1], (F,), F ** -0.5, 0.0625, ((0, 8),), jnp.float32)
    feature_scale = jnp.clip(jnp.exp(math.log(2.0) - 3.6888794 * jax.random.uniform(key_list[2], (F,), jnp.float32) ** steps_of(key_list[2], (F,), ((0, 8),), -0.2, 0.2)), 0.05, 2.0)
    labels = with_ends((jax.random.randint(key_list[3], (SAMPLES,), 0, 2) < 1).astype(jnp.int32), jax.random.fold_in(key_list[3], 1), 0, 1)
    psi = noise(key_list[4], (R_DEV, S), R_DEV ** -0.5, 0.1875)
    phi = noise(key_list[5], (2 * S, S), (2 * S) ** -0.5, 0.25, (), jnp.float32)
    return dict(design=design, theta=theta, feature_scale=feature_scale, labels=labels, psi=psi, phi=phi)


damping = 0.01
shrink_share = 0.05
highest = lax.Precision.HIGHEST

def shrink_weights(range_rows):
    width = range_rows.shape[1]
    moment = jnp.dot(range_rows.T, range_rows, precision=highest)
    ridge = shrink_share * jnp.trace(moment) / width
    factor = jnp.linalg.cholesky(moment + ridge * jnp.eye(width, dtype=jnp.float32))
    return jax.scipy.linalg.solve_triangular(factor, range_rows.T, lower=True)

def reference(design, theta, feature_scale, labels, psi, phi):
    samples = design.shape[0]
    features = design.shape[1]
    scaled_theta = (theta * feature_scale).astype(jnp.bfloat16)
    margins = jnp.dot(design.astype(jnp.float32), scaled_theta.astype(jnp.float32), preferred_element_type=jnp.float32)
    chance = jax.nn.sigmoid(margins)
    weight = chance * (1.0 - chance)
    misfit = (chance - labels.astype(jnp.float32)).astype(jnp.bfloat16)
    gradient = feature_scale * jnp.dot(misfit.astype(jnp.float32), design.astype(jnp.float32), preferred_element_type=jnp.float32) / samples + damping * theta

    def local_sketch(pieces):
        block, block_weight = pieces
        rows_scaled = (block.astype(jnp.float32) * jnp.sqrt(block_weight)[:, None] * feature_scale[None, :]).astype(jnp.bfloat16)
        mixed_cols = jnp.dot(rows_scaled.T.astype(jnp.float32), psi.astype(jnp.float32), preferred_element_type=jnp.float32).astype(jnp.bfloat16)
        range_rows = jnp.dot(rows_scaled.astype(jnp.float32), mixed_cols.astype(jnp.float32), preferred_element_type=jnp.float32)
        leaf_weights = shrink_weights(range_rows).astype(jnp.bfloat16)
        return jnp.dot(leaf_weights.astype(jnp.float32), rows_scaled.astype(jnp.float32), preferred_element_type=jnp.float32)

    def merge_pair(stacked):
        gram = jnp.dot(stacked, stacked.T, precision=highest)
        range_rows = jnp.dot(gram, phi, precision=highest)
        return jnp.dot(shrink_weights(range_rows), stacked, precision=highest)
    sketches = lax.map(local_sketch, (design.reshape(N_ROWS, R_DEV, features), weight.reshape(N_ROWS, R_DEV)))
    for level_index in range(LEVELS):
        pairs_now = sketches.shape[0] // 2
        sketches = lax.map(merge_pair, sketches.reshape(pairs_now, 2 * S, features))
    sketch = sketches[0]
    kernel = jnp.dot(sketch, sketch.T, precision=highest) + damping * samples * jnp.eye(S, dtype=jnp.float32)
    kernel_factor = jnp.linalg.cholesky(kernel)

    def precondition(vector):
        projected = jnp.dot(sketch, vector, precision=highest)
        solved = jax.scipy.linalg.cho_solve((kernel_factor, True), projected)
        return (vector - jnp.dot(solved, sketch, precision=highest)) / damping

    def hessian(vector):
        rounded = (feature_scale * vector).astype(jnp.bfloat16)
        forward_rows = jnp.dot(design.astype(jnp.float32), rounded.astype(jnp.float32), preferred_element_type=jnp.float32)
        inner = (weight * forward_rows).astype(jnp.bfloat16)
        return feature_scale * jnp.dot(inner.astype(jnp.float32), design.astype(jnp.float32), preferred_element_type=jnp.float32) / samples + damping * vector
    solution = jnp.zeros_like(gradient)
    residual = gradient
    search = precondition(residual)
    agreement = jnp.sum(residual * search)
    for turn_index in range(ITERS):
        product = hessian(search)
        step_size = agreement / jnp.sum(search * product)
        solution = solution + step_size * search
        residual = residual - step_size * product
        smoothed = precondition(residual)
        agreement_next = jnp.sum(residual * smoothed)
        search = smoothed + agreement_next / agreement * search
        agreement = agreement_next
    return (solution, sketch)
```

```python
import functools

import jax
import jax.numpy as jnp
from jax import lax
from jax.experimental import pallas as pl
from jax.experimental.pallas import tpu as pltpu
from jax.sharding import PartitionSpec as P

ITERS = 10


damping = 0.01
shrink_share = 0.05
highest = lax.Precision.HIGHEST
LANES = 128
BLOCK = 16
NT = (((1,), (1,)), ((), ()))
NN = (((1,), (0,)), ((), ()))
TN = (((0,), (0,)), ((), ()))


def swapped(value, axis, stride):
    mask = 2**stride
    pairs = [(source, source ^ mask) for source in range(lax.axis_size(axis))]
    return lax.ppermute(value, axis, pairs)


def shrink_weights(range_rows):
    moment = jnp.dot(range_rows.T, range_rows, precision=highest)
    return jnp.dot(inverse_factor(moment, shrink_share), range_rows.T, precision=highest)


def split(value, parts):
    out = []
    for _ in range(parts):
        piece = value.astype(jnp.bfloat16)
        out.append(piece)
        value = value - piece.astype(jnp.float32)
    return out


def factor_kernel(share, m_ref, w_ref, a_ref):
    n = m_ref.shape[0]
    row = lax.broadcasted_iota(jnp.int32, (n, n), 0)
    lane = lax.broadcasted_iota(jnp.int32, (n, n), 1)
    m = m_ref[...]
    diag = jnp.where(row == lane, m, 0.0)
    trace = jnp.sum(jnp.sum(diag, axis=0, keepdims=True), axis=1, keepdims=True)
    a_ref[...] = m + jnp.where(row == lane, share * trace / n, 0.0)
    sub = lax.broadcasted_iota(jnp.int32, (BLOCK, LANES), 0)
    wide_sub = lax.broadcasted_iota(jnp.int32, (BLOCK, n), 0)
    wide_lane = lax.broadcasted_iota(jnp.int32, (BLOCK, n), 1)
    for half in range(n // LANES):
        first_row = half * LANES

        def step(block, carry):
            base = half * LANES + block * BLOCK
            panel = a_ref[pl.ds(pl.multiple_of(base, BLOCK), BLOCK), :]
            tile = panel[:, half * LANES : (half + 1) * LANES]
            tile = pltpu.roll(tile, (LANES - block * BLOCK) % LANES, 1)
            cols = [jnp.broadcast_to(tile[:, m : m + 1], (BLOCK, LANES)) for m in range(BLOCK)]
            inside = (wide_lane >= base) & (wide_lane < base + BLOCK)
            panel = jnp.where(inside, jnp.where(wide_lane - base == wide_sub, 1.0, 0.0), panel)
            scale = jnp.zeros((BLOCK, LANES), jnp.float32)
            for k in range(BLOCK):
                pivot = jnp.broadcast_to(cols[k][k : k + 1], (BLOCK, LANES))
                inverse = 1.0 / pivot
                scale = jnp.where(sub == k, lax.rsqrt(pivot), scale)
                factor = jnp.where(sub > k, cols[k], 0.0) * inverse
                panel = panel - jnp.concatenate([factor] * (n // LANES), 1) * panel[k : k + 1]
                for m in range(k + 1, BLOCK):
                    cols[m] = cols[m] - factor * cols[k][m : m + 1]
            panel = panel * jnp.concatenate([scale] * (n // LANES), 1)
            a_ref[pl.ds(pl.multiple_of(base, BLOCK), BLOCK), :] = panel
            after = jnp.where(wide_lane >= base + BLOCK, panel, 0.0)[:, first_row:]
            l0, l1, l2 = split(after, 3)
            r0, r1, r2 = split(panel, 3)
            left = jnp.concatenate([l0, l0, l1, l0, l1, l2], 0)
            right = jnp.concatenate([r0, r1, r0, r2, r1, r0], 0)
            update = lax.dot_general(left, right, TN, preferred_element_type=jnp.float32)
            old = a_ref[first_row:, :]
            lane_here, row_here = lane[first_row:], row[first_row:]
            gone = (lane_here >= base) & (lane_here < base + BLOCK) & (row_here >= base + BLOCK)
            a_ref[first_row:, :] = jnp.where(gone, 0.0, old) - update
            return carry

        lax.fori_loop(0, LANES // BLOCK, step, 0)
    w_ref[...] = jnp.where(lane <= row, a_ref[...], 0.0)

def inverse_factor(m, share):
    n = m.shape[0]
    return pl.pallas_call(
        functools.partial(factor_kernel, share),
        out_shape=jax.ShapeDtypeStruct((n, n), jnp.float32),
        in_specs=[pl.BlockSpec(memory_space=pltpu.VMEM)],
        out_specs=pl.BlockSpec(memory_space=pltpu.VMEM),
        scratch_shapes=[pltpu.VMEM((n, n), jnp.float32)],
        cost_estimate=pl.CostEstimate(flops=20_000_000, bytes_accessed=600_000, transcendentals=0),
    )(m)


def stacked_splits(row):
    n = row.shape[1]
    high = row.astype(jnp.bfloat16).astype(jnp.float32)
    rest = row - high
    mid = rest.astype(jnp.bfloat16).astype(jnp.float32)
    low = rest - mid
    at = lax.broadcasted_iota(jnp.int32, (8, n), 0)
    full = jnp.where(at == 0, high, jnp.where(at == 1, mid, jnp.where(at == 2, low, 0.0)))
    return full.astype(jnp.bfloat16)


def row_dot(stack, matrices, dims):
    total = None
    for matrix in matrices:
        part = lax.dot_general(stack, matrix, dims, preferred_element_type=jnp.float32)
        total = part if total is None else total + part
    return jnp.sum(total, axis=0, keepdims=True)


def put_scalars(values):
    at = lax.broadcasted_iota(jnp.int32, (1, LANES), 1)
    row = jnp.zeros((1, LANES), jnp.float32)
    for index, value in enumerate(values):
        row = jnp.where(at == index, value, row)
    return row


def total(row):
    return jnp.sum(row, axis=1, keepdims=True)


def forward_kernel(samples, first, *refs):
    if first:
        (grad_ref, q_ref, scale_ref, design_ref, s0_ref, s1_ref, inv_ref, vec_out, small_out, msg_out) = refs
        r = grad_ref[...]
        x = jnp.zeros_like(r)
        q = q_ref[...]
    else:
        (at_ref, msg_ref, vec_ref, small_ref, scales_ref, scale_ref, design_ref, s0_ref, s1_ref, inv_ref, vec_out, small_out, msg_out) = refs
        groups, n_col = msg_ref.shape[0], msg_ref.shape[1]
        feats = scale_ref.shape[1]
        width = inv_ref.shape[1]
        here = at_ref[0]
        squares = jnp.zeros((1, feats), jnp.float32)
        tail = jnp.zeros((1, width + LANES), jnp.float32)
        for col in range(n_col):
            back = msg_ref[0, col, :, :feats]
            tail = tail + msg_ref[0, col, :, feats:]
            for group in range(1, groups):
                back = back + msg_ref[group, col, :, :feats]
                tail = tail + msg_ref[group, col, :, feats:]
            pulled = scales_ref[col] * back
            squares = squares + pulled * pulled
        back = msg_ref[0, here, :, :feats]
        for group in range(1, groups):
            back = back + msg_ref[group, here, :, :feats]
        x, r, p = vec_ref[0:1], vec_ref[1:2], vec_ref[2:3]
        q, sp = small_ref[0:1], small_ref[1:2]
        agreement, length = small_ref[2:3, 0:1], small_ref[2:3, 1:2]
        bending = tail[:, width : width + 1] / (n_col * samples)
        curvature = bending + damping * length
        step = agreement / curvature
        product = scale_ref[...] * back / samples + damping * p
        x = x + step * p
        r = r - step * product
        pressed = tail[:, :width] / samples + damping * sp
        q = q - step * pressed
    inv = split(inv_ref[...], 3)
    s = row_dot(stacked_splits(q), inv, NN)
    s0, s1 = s0_ref[...], s1_ref[...]
    z = (r - row_dot(stacked_splits(s), (s0, s1), NN)) / damping
    if first:
        p = z
    else:
        solved = row_dot(stacked_splits(pressed), inv, NN)
        norm = total(squares) / (samples * samples) + 2.0 * damping * bending + damping * damping * length
        bent = (norm - total(pressed * solved)) / damping
        p = z + (step * step * bent / agreement - 1.0) * p
    rounded = (scale_ref[...] * p).astype(jnp.bfloat16)
    ahead = lax.dot_general(
        jnp.broadcast_to(rounded, (8, rounded.shape[1])), design_ref[...], NT,
        preferred_element_type=jnp.float32,
    )[0:1]
    sp = row_dot(stacked_splits(p), (s0, s1), NT)
    scalars = put_scalars((total(r * z), total(p * p)))
    message = jnp.concatenate([ahead, sp, scalars], axis=1)
    for col in range(msg_out.shape[0]):
        msg_out[col] = message
    vec_out[...] = jnp.zeros_like(vec_out)
    vec_out[0:1] = x
    vec_out[1:2] = r
    vec_out[2:3] = p
    small_out[...] = jnp.zeros_like(small_out)
    small_out[0:1] = q


def backward_kernel(last, *refs):
    if last:
        (msg_ref, small_ref, weight_ref, small_out, bend_out) = refs
    else:
        (msg_ref, small_ref, weight_ref, scale_ref, design_ref, s0_ref, s1_ref, small_out, msg_out) = refs
    rows = weight_ref.shape[1]
    width = small_ref.shape[1]
    sums = msg_ref[0]
    for col in range(1, msg_ref.shape[0]):
        sums = sums + msg_ref[col]
    y = sums[:, :rows]
    rest = sums[:, rows + width :]
    inner = (weight_ref[...] * y).astype(jnp.bfloat16)
    bend = total(inner.astype(jnp.float32) * y)
    at = lax.broadcasted_iota(jnp.int32, (1, width), 1)
    small_out[...] = jnp.zeros_like(small_out)
    small_out[0:1] = small_ref[0:1]
    small_out[1:2] = sums[:, rows : rows + width]
    small_out[2:3] = jnp.where(at == 0, rest[:, 0:1], jnp.where(at == 1, rest[:, 1:2], 0.0))
    if last:
        bend_out[...] = put_scalars((bend,))
        return
    back = lax.dot_general(
        jnp.broadcast_to(inner, (8, rows)), design_ref[...], NN, preferred_element_type=jnp.float32
    )[0:1]
    sb = row_dot(stacked_splits(scale_ref[...] * back), (s0_ref[...], s1_ref[...]), NT)
    message = jnp.concatenate([back, sb, put_scalars((bend,))], axis=1)
    for group in range(msg_out.shape[0]):
        for col in range(msg_out.shape[1]):
            msg_out[group, col] = message


def call(kernel, shapes, args, smem=0, flops=4_000_000):
    specs = [pl.BlockSpec(memory_space=pltpu.SMEM)] * smem
    specs += [pl.BlockSpec(memory_space=pltpu.VMEM)] * (len(args) - smem)
    return pl.pallas_call(
        kernel,
        out_shape=[jax.ShapeDtypeStruct(shape, jnp.float32) for shape in shapes],
        in_specs=specs,
        out_specs=[pl.BlockSpec(memory_space=pltpu.VMEM)] * len(shapes),
        cost_estimate=pl.CostEstimate(flops=flops, bytes_accessed=1_000_000, transcendentals=0),
    )(*args)


def heard_cols(row):
    n_col = lax.axis_size("cols")
    return lax.all_to_all(jnp.broadcast_to(row[None], (n_col, *row.shape)), "cols", 0, 0)


def summed_cols(row):
    return jnp.sum(heard_cols(row), 0)


def solve(design, weight, feature_scale, scales, gradient, sketch, inverse, samples):
    n_row, n_col = lax.axis_size("rows"), lax.axis_size("cols")
    rows, feats = design.shape
    width = sketch.shape[0]
    scale = feature_scale[None]
    high = lax.reduce_precision(sketch, 8, 7)
    s0, s1 = high.astype(jnp.bfloat16), (sketch - high).astype(jnp.bfloat16)
    weight = weight[None]
    q = summed_cols(jnp.dot(gradient[None], sketch.T, precision=highest))
    here = lax.axis_index("cols").astype(jnp.int32)[None]
    vec_shape, small_shape = (8, feats), (8, width)
    ahead_shape = (n_col, 1, rows + width + LANES)
    back_shape = (n_row, n_col, 1, feats + width + LANES)
    vec, small, message = call(
        functools.partial(forward_kernel, samples, True),
        (vec_shape, small_shape, ahead_shape),
        (gradient[None], q, scale, design, s0, s1, inverse),
    )
    for turn in range(ITERS):
        message = lax.all_to_all(message, "cols", 0, 0)
        if turn + 1 == ITERS:
            break
        small, message = call(
            functools.partial(backward_kernel, False),
            (small_shape, back_shape),
            (message, small, weight, scale, design, s0, s1),
        )
        message = message.reshape(n_row * n_col, 1, -1)
        message = lax.all_to_all(message, ("rows", "cols"), 0, 0).reshape(back_shape)
        vec, small, message = call(
            functools.partial(forward_kernel, samples, False),
            (vec_shape, small_shape, ahead_shape),
            (here, message, vec, small, scales, scale, design, s0, s1, inverse),
            smem=1,
        )
    small, bend = call(
        functools.partial(backward_kernel, True),
        (small_shape, (1, LANES)),
        (message, small, weight),
    )
    bend = lax.psum(bend, "rows")[0, 0]
    curvature = bend / samples + damping * small[2, 1]
    return vec[0] + small[2, 0] / curvature * vec[2]


def on_device(design, theta, feature_scale, labels, psi, phi):
    row_devices = lax.axis_size("rows")
    samples = design.shape[0] * row_devices
    width = psi.shape[1]
    scaled_theta = (theta * feature_scale).astype(jnp.bfloat16)
    part = jnp.dot(design, scaled_theta, preferred_element_type=jnp.float32)
    rows = part.shape[0]
    heard = heard_cols(jnp.concatenate([part, feature_scale])[None])
    margins = jnp.sum(heard[:, 0, :rows], 0)
    scales = heard[:, :, rows:]
    chance = jax.nn.sigmoid(margins)
    weight = chance * (1.0 - chance)
    misfit = (chance - labels.astype(jnp.float32)).astype(jnp.bfloat16)
    summed_grad = lax.psum(jnp.dot(misfit, design, preferred_element_type=jnp.float32), "rows")
    gradient = feature_scale * summed_grad / samples + damping * theta
    rows_scaled = (
        design.astype(jnp.float32) * jnp.sqrt(weight)[:, None] * feature_scale[None, :]
    ).astype(jnp.bfloat16)
    mixed_cols = jnp.einsum(
        "rf,rs->fs", rows_scaled, psi, preferred_element_type=jnp.float32
    ).astype(jnp.bfloat16)
    range_rows = lax.psum(
        jnp.dot(rows_scaled, mixed_cols, preferred_element_type=jnp.float32), "cols"
    )
    leaf_weights = shrink_weights(range_rows).astype(jnp.bfloat16)
    sketch = jnp.dot(leaf_weights, rows_scaled, preferred_element_type=jnp.float32)
    position = lax.axis_index("rows")
    for level_bit in range(row_devices.bit_length() - 1):
        partner = swapped(sketch, "rows", level_bit)
        first_low = position // (1 << level_bit) % 2 == 0
        lower_half = jnp.where(first_low, sketch, partner)
        upper_half = jnp.where(first_low, partner, sketch)
        stacked = jnp.concatenate([lower_half, upper_half], 0)
        gram = lax.psum(jnp.dot(stacked, stacked.T, precision=highest), "cols")
        range_rows = jnp.dot(gram, phi, precision=highest)
        sketch = jnp.dot(shrink_weights(range_rows), stacked, precision=highest)
    kernel_part = lax.psum(jnp.dot(sketch, sketch.T, precision=highest), "cols")
    kernel = kernel_part + damping * samples * jnp.eye(width, dtype=jnp.float32)
    factor = inverse_factor(kernel, 0.0)
    inverse = jnp.dot(factor.T, factor, precision=highest)
    newton = solve(design, weight, feature_scale, scales, gradient, sketch, inverse, samples)
    return (newton, sketch)


def solution(mesh):
    in_specs = (P("rows", "cols"), P("cols"), P("cols"), P("rows"), P(), P())
    out_specs = (P("cols"), P(None, "cols"))
    return jax.shard_map(
        on_device, mesh=mesh, in_specs=in_specs, out_specs=out_specs, check_vma=False
    )
```

```python
import functools

import jax
import jax.numpy as jnp
from jax import lax
from jax.experimental import pallas as pl
from jax.experimental.pallas import tpu as pltpu
from jax.sharding import PartitionSpec as P

ITERS = 10


damping = 0.01
shrink_share = 0.05
highest = lax.Precision.HIGHEST
LANES = 128
BLOCK = 16
VMEM_LIMIT = 16 * 1024 * 1024
NT = (((1,), (1,)), ((), ()))
NN = (((1,), (0,)), ((), ()))
TN = (((0,), (0,)), ((), ()))


def swapped(value, axis, stride):
    mask = 2**stride
    pairs = [(source, source ^ mask) for source in range(lax.axis_size(axis))]
    return lax.ppermute(value, axis, pairs)


def shrink_weights(range_rows):
    moment = jnp.dot(range_rows.T, range_rows, precision=highest)
    return jnp.dot(inverse_factor(moment, shrink_share), range_rows.T, precision=highest)


def scattered_cols(part):
    n_col = lax.axis_size("cols")
    blocks = part.reshape(n_col, part.shape[0] // n_col, part.shape[1])
    return jnp.sum(lax.all_to_all(blocks, "cols", 0, 0), 0)


def summed_blocks(part):
    n_col = lax.axis_size("cols")
    block = scattered_cols(part)
    sent = jnp.broadcast_to(block[None], (n_col, *block.shape))
    return lax.all_to_all(sent, "cols", 0, 0).reshape(part.shape)


def in_order(first, mine, other):
    return jnp.where(first, mine, other), jnp.where(first, other, mine)


def rows_at(value, index, count):
    size = value.shape[0] // count
    return lax.dynamic_slice_in_dim(value, index * size, size, 0)


def leaf_gram(leaf, position):
    width = leaf.shape[0]
    low = position % 2 == 0
    lower, upper = in_order(low, leaf, swapped(leaf, "rows", 0))
    piece = rows_at(lower, position % 2, 2)
    share = jnp.concatenate([gram_of(leaf, leaf), gram_of(piece, upper)], 0)
    share = summed_blocks(share)
    first, second = in_order(low, share, swapped(share, "rows", 0))
    cross = jnp.concatenate([first[width:], second[width:]], 0)
    return jnp.concatenate([lower, upper], 0), first[:width], second[:width], cross


def gram_of(left, right):
    return lax.dot_general(left, right, NT, precision=highest)


def merge_gram(sketch, gram, position, level):
    n_row, n_col = lax.axis_size("rows"), lax.axis_size("cols")
    width, feats = sketch.shape
    group = 1 << level
    both = jnp.concatenate([rows_at(sketch, position % group, group), rows_at(gram, position % group, group)], 1)
    both = swapped(both, "rows", level)
    for bit in range(level):
        first, second = in_order(position // (1 << bit) % 2 == 0, both, swapped(both, "rows", bit))
        both = jnp.concatenate([first, second], 0)
    low = position // group % 2 == 0
    lower, upper = in_order(low, sketch, both[:, :feats])
    first, second = in_order(low, gram, both[:, feats:])
    part = gram_of(rows_at(lower, position % (2 * group), 2 * group), upper)
    block = scattered_cols(part)
    sent = jnp.broadcast_to(block[None], (n_row * n_col, *block.shape))
    heard = lax.all_to_all(sent, ("rows", "cols"), 0, 0).reshape(n_row, -1, width)
    cross = lax.dynamic_slice_in_dim(heard, position // (2 * group) * (2 * group), 2 * group, 0)
    return jnp.concatenate([lower, upper], 0), first, second, cross.reshape(width, width)


def split(value, parts):
    out = []
    for _ in range(parts):
        piece = value.astype(jnp.bfloat16)
        out.append(piece)
        value = value - piece.astype(jnp.float32)
    return out


def factor_kernel(share, m_ref, w_ref, a_ref):
    n = m_ref.shape[0]
    row = lax.broadcasted_iota(jnp.int32, (n, n), 0)
    lane = lax.broadcasted_iota(jnp.int32, (n, n), 1)
    m = m_ref[...]
    diag = jnp.where(row == lane, m, 0.0)
    trace = jnp.sum(jnp.sum(diag, axis=0, keepdims=True), axis=1, keepdims=True)
    a_ref[...] = m + jnp.where(row == lane, share * trace / n, 0.0)
    sub = lax.broadcasted_iota(jnp.int32, (BLOCK, LANES), 0)
    wide_sub = lax.broadcasted_iota(jnp.int32, (BLOCK, n), 0)
    wide_lane = lax.broadcasted_iota(jnp.int32, (BLOCK, n), 1)
    for half in range(n // LANES):
        first_row = half * LANES

        def step(block, carry):
            base = half * LANES + block * BLOCK
            panel = a_ref[pl.ds(pl.multiple_of(base, BLOCK), BLOCK), :]
            tile = panel[:, half * LANES : (half + 1) * LANES]
            tile = pltpu.roll(tile, (LANES - block * BLOCK) % LANES, 1)
            cols = [jnp.broadcast_to(tile[:, m : m + 1], (BLOCK, LANES)) for m in range(BLOCK)]
            inside = (wide_lane >= base) & (wide_lane < base + BLOCK)
            panel = jnp.where(inside, jnp.where(wide_lane - base == wide_sub, 1.0, 0.0), panel)
            scale = jnp.zeros((BLOCK, LANES), jnp.float32)
            for k in range(BLOCK):
                pivot = jnp.broadcast_to(cols[k][k : k + 1], (BLOCK, LANES))
                inverse = 1.0 / pivot
                scale = jnp.where(sub == k, lax.rsqrt(pivot), scale)
                factor = jnp.where(sub > k, cols[k], 0.0) * inverse
                panel = panel - jnp.concatenate([factor] * (n // LANES), 1) * panel[k : k + 1]
                for m in range(k + 1, BLOCK):
                    cols[m] = cols[m] - factor * cols[k][m : m + 1]
            panel = panel * jnp.concatenate([scale] * (n // LANES), 1)
            a_ref[pl.ds(pl.multiple_of(base, BLOCK), BLOCK), :] = panel
            after = jnp.where(wide_lane >= base + BLOCK, panel, 0.0)[:, first_row:]
            l0, l1, l2 = split(after, 3)
            r0, r1, r2 = split(panel, 3)
            left = jnp.concatenate([l0, l0, l1, l0, l1, l2], 0)
            right = jnp.concatenate([r0, r1, r0, r2, r1, r0], 0)
            update = lax.dot_general(left, right, TN, preferred_element_type=jnp.float32)
            old = a_ref[first_row:, :]
            lane_here, row_here = lane[first_row:], row[first_row:]
            gone = (lane_here >= base) & (lane_here < base + BLOCK) & (row_here >= base + BLOCK)
            a_ref[first_row:, :] = jnp.where(gone, 0.0, old) - update
            return carry

        lax.fori_loop(0, LANES // BLOCK, step, 0)
    w_ref[...] = jnp.where(lane <= row, a_ref[...], 0.0)

def inverse_factor(m, share):
    n = m.shape[0]
    return pl.pallas_call(
        functools.partial(factor_kernel, share),
        out_shape=jax.ShapeDtypeStruct((n, n), jnp.float32),
        in_specs=[pl.BlockSpec(memory_space=pltpu.VMEM)],
        out_specs=pl.BlockSpec(memory_space=pltpu.VMEM),
        scratch_shapes=[pltpu.VMEM((n, n), jnp.float32)],
        compiler_params=pltpu.CompilerParams(vmem_limit_bytes=VMEM_LIMIT),
        cost_estimate=pl.CostEstimate(flops=20_000_000, bytes_accessed=600_000, transcendentals=0),
    )(m)


def stacked_splits(row):
    n = row.shape[1]
    high = row.astype(jnp.bfloat16).astype(jnp.float32)
    rest = row - high
    mid = rest.astype(jnp.bfloat16).astype(jnp.float32)
    low = rest - mid
    at = lax.broadcasted_iota(jnp.int32, (8, n), 0)
    full = jnp.where(at == 0, high, jnp.where(at == 1, mid, jnp.where(at == 2, low, 0.0)))
    return full.astype(jnp.bfloat16)


def row_dot(stack, matrices, dims):
    total = None
    for matrix in matrices:
        part = lax.dot_general(stack, matrix, dims, preferred_element_type=jnp.float32)
        total = part if total is None else total + part
    return jnp.sum(total, axis=0, keepdims=True)


def put_scalars(values):
    at = lax.broadcasted_iota(jnp.int32, (1, LANES), 1)
    row = jnp.zeros((1, LANES), jnp.float32)
    for index, value in enumerate(values):
        row = jnp.where(at == index, value, row)
    return row


def total(row):
    return jnp.sum(row, axis=1, keepdims=True)


def forward_kernel(samples, first, *refs):
    if first:
        (grad_ref, q_ref, scale_ref, design_ref, s0_ref, s1_ref, inv_ref, vec_out, small_out, msg_out) = refs
        r = grad_ref[...]
        x = jnp.zeros_like(r)
        q = q_ref[...]
    else:
        (at_ref, msg_ref, vec_ref, small_ref, scales_ref, scale_ref, design_ref, s0_ref, s1_ref, inv_ref, vec_out, small_out, msg_out) = refs
        groups, n_col = msg_ref.shape[0], msg_ref.shape[1]
        feats = scale_ref.shape[1]
        width = inv_ref.shape[1]
        here = at_ref[0]
        squares = jnp.zeros((1, feats), jnp.float32)
        tail = jnp.zeros((1, width + LANES), jnp.float32)
        for col in range(n_col):
            back = msg_ref[0, col, :, :feats]
            tail = tail + msg_ref[0, col, :, feats:]
            for group in range(1, groups):
                back = back + msg_ref[group, col, :, :feats]
                tail = tail + msg_ref[group, col, :, feats:]
            pulled = scales_ref[col] * back
            squares = squares + pulled * pulled
        back = msg_ref[0, here, :, :feats]
        for group in range(1, groups):
            back = back + msg_ref[group, here, :, :feats]
        x, r, p = vec_ref[0:1], vec_ref[1:2], vec_ref[2:3]
        q, sp = small_ref[0:1], small_ref[1:2]
        agreement, length = small_ref[2:3, 0:1], small_ref[2:3, 1:2]
        bending = tail[:, width : width + 1] / (n_col * samples)
        curvature = bending + damping * length
        step = agreement / curvature
        product = scale_ref[...] * back / samples + damping * p
        x = x + step * p
        r = r - step * product
        pressed = tail[:, :width] / samples + damping * sp
        q = q - step * pressed
    inv = split(inv_ref[...], 3)
    s = row_dot(stacked_splits(q), inv, NN)
    s0, s1 = s0_ref[...], s1_ref[...]
    z = (r - row_dot(stacked_splits(s), (s0, s1), NN)) / damping
    if first:
        p = z
    else:
        solved = row_dot(stacked_splits(pressed), inv, NN)
        norm = total(squares) / (samples * samples) + 2.0 * damping * bending + damping * damping * length
        bent = (norm - total(pressed * solved)) / damping
        p = z + (step * step * bent / agreement - 1.0) * p
    rounded = (scale_ref[...] * p).astype(jnp.bfloat16)
    ahead = lax.dot_general(
        jnp.broadcast_to(rounded, (8, rounded.shape[1])), design_ref[...], NT,
        preferred_element_type=jnp.float32,
    )[0:1]
    sp = row_dot(stacked_splits(p), (s0, s1), NT)
    scalars = put_scalars((total(r * z), total(p * p)))
    message = jnp.concatenate([ahead, sp, scalars], axis=1)
    for col in range(msg_out.shape[0]):
        msg_out[col] = message
    vec_out[...] = jnp.zeros_like(vec_out)
    vec_out[0:1] = x
    vec_out[1:2] = r
    vec_out[2:3] = p
    small_out[...] = jnp.zeros_like(small_out)
    small_out[0:1] = q


def backward_kernel(last, *refs):
    if last:
        (msg_ref, small_ref, weight_ref, small_out, bend_out) = refs
    else:
        (msg_ref, small_ref, weight_ref, scale_ref, design_ref, s0_ref, s1_ref, small_out, msg_out) = refs
    rows = weight_ref.shape[1]
    width = small_ref.shape[1]
    sums = msg_ref[0]
    for col in range(1, msg_ref.shape[0]):
        sums = sums + msg_ref[col]
    y = sums[:, :rows]
    rest = sums[:, rows + width :]
    inner = (weight_ref[...] * y).astype(jnp.bfloat16)
    bend = total(inner.astype(jnp.float32) * y)
    at = lax.broadcasted_iota(jnp.int32, (1, width), 1)
    small_out[...] = jnp.zeros_like(small_out)
    small_out[0:1] = small_ref[0:1]
    small_out[1:2] = sums[:, rows : rows + width]
    small_out[2:3] = jnp.where(at == 0, rest[:, 0:1], jnp.where(at == 1, rest[:, 1:2], 0.0))
    if last:
        bend_out[...] = put_scalars((bend,))
        return
    back = lax.dot_general(
        jnp.broadcast_to(inner, (8, rows)), design_ref[...], NN, preferred_element_type=jnp.float32
    )[0:1]
    sb = row_dot(stacked_splits(scale_ref[...] * back), (s0_ref[...], s1_ref[...]), NT)
    message = jnp.concatenate([back, sb, put_scalars((bend,))], axis=1)
    for group in range(msg_out.shape[0]):
        for col in range(msg_out.shape[1]):
            msg_out[group, col] = message


def call(kernel, shapes, args, smem=0, flops=4_000_000):
    specs = [pl.BlockSpec(memory_space=pltpu.SMEM)] * smem
    specs += [pl.BlockSpec(memory_space=pltpu.VMEM)] * (len(args) - smem)
    return pl.pallas_call(
        kernel,
        out_shape=[jax.ShapeDtypeStruct(shape, jnp.float32) for shape in shapes],
        in_specs=specs,
        out_specs=[pl.BlockSpec(memory_space=pltpu.VMEM)] * len(shapes),
        compiler_params=pltpu.CompilerParams(vmem_limit_bytes=VMEM_LIMIT),
        cost_estimate=pl.CostEstimate(flops=flops, bytes_accessed=1_000_000, transcendentals=0),
    )(*args)


def heard_cols(row):
    n_col = lax.axis_size("cols")
    return lax.all_to_all(jnp.broadcast_to(row[None], (n_col, *row.shape)), "cols", 0, 0)


def summed_cols(row):
    return jnp.sum(heard_cols(row), 0)


def solve(design, weight, feature_scale, scales, gradient, sketch, q, inverse, samples):
    n_row, n_col = lax.axis_size("rows"), lax.axis_size("cols")
    rows, feats = design.shape
    width = sketch.shape[0]
    scale = feature_scale[None]
    high = lax.reduce_precision(sketch, 8, 7)
    s0, s1 = high.astype(jnp.bfloat16), (sketch - high).astype(jnp.bfloat16)
    weight = weight[None]
    here = lax.axis_index("cols").astype(jnp.int32)[None]
    vec_shape, small_shape = (8, feats), (8, width)
    ahead_shape = (n_col, 1, rows + width + LANES)
    back_shape = (n_row, n_col, 1, feats + width + LANES)
    vec, small, message = call(
        functools.partial(forward_kernel, samples, True),
        (vec_shape, small_shape, ahead_shape),
        (gradient[None], q, scale, design, s0, s1, inverse),
    )
    for turn in range(ITERS):
        message = lax.all_to_all(message, "cols", 0, 0)
        if turn + 1 == ITERS:
            break
        small, message = call(
            functools.partial(backward_kernel, False),
            (small_shape, back_shape),
            (message, small, weight, scale, design, s0, s1),
        )
        message = message.reshape(n_row * n_col, 1, -1)
        message = lax.all_to_all(message, ("rows", "cols"), 0, 0).reshape(back_shape)
        vec, small, message = call(
            functools.partial(forward_kernel, samples, False),
            (vec_shape, small_shape, ahead_shape),
            (here, message, vec, small, scales, scale, design, s0, s1, inverse),
            smem=1,
        )
    small, bend = call(
        functools.partial(backward_kernel, True),
        (small_shape, (1, LANES)),
        (message, small, weight),
    )
    bend = lax.psum(bend, "rows")[0, 0]
    curvature = bend / samples + damping * small[2, 1]
    return vec[0] + small[2, 0] / curvature * vec[2]


def on_device(design, theta, feature_scale, labels, psi, phi):
    row_devices = lax.axis_size("rows")
    samples = design.shape[0] * row_devices
    width = psi.shape[1]
    scaled_theta = (theta * feature_scale).astype(jnp.bfloat16)
    part = jnp.dot(design, scaled_theta, preferred_element_type=jnp.float32)
    rows = part.shape[0]
    heard = heard_cols(jnp.concatenate([part, feature_scale])[None])
    margins = jnp.sum(heard[:, 0, :rows], 0)
    scales = heard[:, :, rows:]
    chance = jax.nn.sigmoid(margins)
    weight = chance * (1.0 - chance)
    misfit = (chance - labels.astype(jnp.float32)).astype(jnp.bfloat16)
    summed_grad = lax.psum(jnp.dot(misfit, design, preferred_element_type=jnp.float32), "rows")
    gradient = feature_scale * summed_grad / samples + damping * theta
    rows_scaled = (
        design.astype(jnp.float32) * jnp.sqrt(weight)[:, None] * feature_scale[None, :]
    ).astype(jnp.bfloat16)
    mixed_cols = jnp.einsum(
        "rf,rs->fs", rows_scaled, psi, preferred_element_type=jnp.float32
    ).astype(jnp.bfloat16)
    range_rows = summed_blocks(
        jnp.dot(rows_scaled, mixed_cols, preferred_element_type=jnp.float32)
    )
    leaf_weights = shrink_weights(range_rows).astype(jnp.bfloat16)
    sketch = jnp.dot(leaf_weights, rows_scaled, preferred_element_type=jnp.float32)
    position = lax.axis_index("rows")
    for level in range(row_devices.bit_length() - 1):
        if level == 0:
            stacked, first, second, cross = leaf_gram(sketch, position)
        else:
            stacked, first, second, cross = merge_gram(sketch, gram, position, level)
        full = jnp.concatenate(
            [jnp.concatenate([first, cross], 1), jnp.concatenate([cross.T, second], 1)], 0
        )
        weights = shrink_weights(jnp.dot(full, phi, precision=highest))
        sketch = jnp.dot(weights, stacked, precision=lax.Precision.HIGH)
        gram = gram_of(jnp.dot(weights, full, precision=highest), weights)
    felt = summed_cols(gram_of(gradient[None], stacked))
    q = gram_of(felt, weights)
    kernel = gram + damping * samples * jnp.eye(width, dtype=jnp.float32)
    factor = inverse_factor(kernel, 0.0)
    inverse = jnp.dot(factor.T, factor, precision=highest)
    newton = solve(design, weight, feature_scale, scales, gradient, sketch, q, inverse, samples)
    return (newton, sketch)


def solution(mesh):
    in_specs = (P("rows", "cols"), P("cols"), P("cols"), P("rows"), P(), P())
    out_specs = (P("cols"), P(None, "cols"))
    return jax.shard_map(
        on_device, mesh=mesh, in_specs=in_specs, out_specs=out_specs, check_vma=False
    )
```

```python
import functools

import jax
import jax.numpy as jnp
from jax import lax
from jax.experimental import pallas as pl
from jax.experimental.pallas import tpu as pltpu
from jax.sharding import PartitionSpec as P

ITERS = 10


damping = 0.01
shrink_share = 0.05
highest = lax.Precision.HIGHEST
LANES = 128
BLOCK = 32
VMEM_LIMIT = 16 * 1024 * 1024
NT = (((1,), (1,)), ((), ()))
NN = (((1,), (0,)), ((), ()))
TN = (((0,), (0,)), ((), ()))


def swapped(value, axis, stride):
    mask = 2**stride
    pairs = [(source, source ^ mask) for source in range(lax.axis_size(axis))]
    return lax.ppermute(value, axis, pairs)


def shrink_weights(range_rows):
    moment = jnp.dot(range_rows.T, range_rows, precision=highest)
    return jnp.dot(inverse_factor(moment, shrink_share), range_rows.T, precision=lax.Precision.HIGH)


def scattered_cols(part):
    n_col = lax.axis_size("cols")
    blocks = part.reshape(n_col, part.shape[0] // n_col, part.shape[1])
    return jnp.sum(lax.all_to_all(blocks, "cols", 0, 0), 0)


def summed_blocks(part):
    n_col = lax.axis_size("cols")
    block = scattered_cols(part)
    sent = jnp.broadcast_to(block[None], (n_col, *block.shape))
    return lax.all_to_all(sent, "cols", 0, 0).reshape(part.shape)


def in_order(first, mine, other):
    return jnp.where(first, mine, other), jnp.where(first, other, mine)


def rows_at(value, index, count):
    size = value.shape[0] // count
    return lax.dynamic_slice_in_dim(value, index * size, size, 0)


def leaf_gram(leaf, grad_sum, position):
    width = leaf.shape[0]
    low = position % 2 == 0
    lower, upper = in_order(low, leaf, swapped(leaf, "rows", 0))
    piece = rows_at(lower, position % 2, 2)
    share = jnp.concatenate([gram_of(leaf, leaf), gram_of(piece, upper)], 0)
    grad_sum = grad_sum + swapped(grad_sum, "rows", 0)
    share, grad_sum = lax.optimization_barrier((share, grad_sum))
    share = summed_blocks(share)
    first, second = in_order(low, share, swapped(share, "rows", 0))
    cross = jnp.concatenate([first[width:], second[width:]], 0)
    return jnp.concatenate([lower, upper], 0), first[:width], second[:width], cross, grad_sum


def gram_of(left, right):
    return lax.dot_general(left, right, NT, precision=lax.Precision.HIGH)


def merge_gram(sketch, gram, grad_sum, gradient_of, weight, position, level):
    n_row, n_col = lax.axis_size("rows"), lax.axis_size("cols")
    width, feats = sketch.shape
    group = 1 << level
    last = 2 * group == n_row
    both = jnp.concatenate([rows_at(sketch, position % group, group), rows_at(gram, position % group, group)], 1)
    grad_other = swapped(grad_sum, "rows", level)
    both, grad_other = lax.optimization_barrier((swapped(both, "rows", level), grad_other))
    grad_sum = grad_sum + grad_other
    gradient = gradient_of(grad_sum)
    for bit in range(level):
        first, second = in_order(position // (1 << bit) % 2 == 0, both, swapped(both, "rows", bit))
        both = jnp.concatenate([first, second], 0)
    low = position // group % 2 == 0
    lower, upper = in_order(low, sketch, both[:, :feats])
    first, second = in_order(low, gram, both[:, feats:])
    stacked = jnp.concatenate([lower, upper], 0)
    part = gram_of(rows_at(lower, position % (2 * group), 2 * group), upper)
    block = scattered_cols(part)
    pieces = [block.reshape(1, -1)]
    if last:
        weight_piece = rows_at(weight, lax.axis_index("cols"), n_col)
        pieces += [gram_of(gradient[None], stacked), weight_piece[None]]
    sent = jnp.concatenate(pieces, 1)
    sent = jnp.broadcast_to(sent[None], (n_row * n_col, *sent.shape))
    heard = lax.all_to_all(sent, ("rows", "cols"), 0, 0).reshape(n_row, n_col, -1)
    start = position // (2 * group) * (2 * group)
    cross = lax.dynamic_slice_in_dim(heard[:, :, : block.size], start, 2 * group, 0)
    felt, weights = None, None
    if last:
        felt = jnp.sum(heard[0, :, block.size : block.size + 2 * width], 0)[None]
        weights = heard[:, :, block.size + 2 * width :].reshape(n_row, 1, -1)
    return stacked, first, second, cross.reshape(width, width), grad_sum, felt, weights


def split(value, parts):
    out = []
    for _ in range(parts):
        piece = value.astype(jnp.bfloat16)
        out.append(piece)
        value = value - piece.astype(jnp.float32)
    return out


def factor_kernel(share, m_ref, w_ref, a_ref):
    n = m_ref.shape[0]
    row = lax.broadcasted_iota(jnp.int32, (n, n), 0)
    lane = lax.broadcasted_iota(jnp.int32, (n, n), 1)
    m = m_ref[...]
    diag = jnp.where(row == lane, m, 0.0)
    trace = jnp.sum(jnp.sum(diag, axis=0, keepdims=True), axis=1, keepdims=True)
    a_ref[...] = m / trace + jnp.where(row == lane, share / n, 0.0)
    sub = lax.broadcasted_iota(jnp.int32, (BLOCK, LANES), 0)
    wide_sub = lax.broadcasted_iota(jnp.int32, (BLOCK, n), 0)
    wide_lane = lax.broadcasted_iota(jnp.int32, (BLOCK, n), 1)
    for half in range(n // LANES):
        first_row = half * LANES

        def step(block, carry):
            base = half * LANES + block * BLOCK
            panel = a_ref[pl.ds(pl.multiple_of(base, BLOCK), BLOCK), :]
            tile = panel[:, half * LANES : (half + 1) * LANES]
            tile = pltpu.roll(tile, (LANES - block * BLOCK) % LANES, 1)
            cols = [jnp.broadcast_to(tile[:, m : m + 1], (BLOCK, LANES)) for m in range(BLOCK)]
            inside = (wide_lane >= base) & (wide_lane < base + BLOCK)
            panel = jnp.where(inside, jnp.where(wide_lane - base == wide_sub, 1.0, 0.0), panel)
            scale = jnp.zeros((BLOCK, LANES), jnp.float32)
            for k in range(0, BLOCK, 2):
                top, low = cols[k], cols[k + 1]
                a = jnp.broadcast_to(top[k : k + 1], (BLOCK, LANES))
                b = jnp.broadcast_to(top[k + 1 : k + 2], (BLOCK, LANES))
                c = jnp.broadcast_to(low[k + 1 : k + 2], (BLOCK, LANES))
                det = a * c - b * b
                inv_a, inv_det = 1.0 / a, 1.0 / det
                scale = jnp.where(sub == k, lax.rsqrt(a), jnp.where(sub == k + 1, lax.rsqrt(det * inv_a), scale))
                first = jnp.where(sub > k, top, 0.0) * inv_a
                low = low - first * b
                second = jnp.where(sub > k + 1, low, 0.0) * (a * inv_det)
                panel = panel - jnp.concatenate([first] * (n // LANES), 1) * panel[k : k + 1]
                panel = panel - jnp.concatenate([second] * (n // LANES), 1) * panel[k + 1 : k + 2]
                for m in range(k + 2, BLOCK):
                    cols[m] = cols[m] - (first * top[m : m + 1] + second * low[m : m + 1])
            panel = panel * jnp.concatenate([scale] * (n // LANES), 1)
            a_ref[pl.ds(pl.multiple_of(base, BLOCK), BLOCK), :] = panel
            after = jnp.where(wide_lane >= base + BLOCK, panel, 0.0)[:, first_row:]
            l0, l1, l2 = split(after, 3)
            r0, r1, r2 = split(panel, 3)
            left = jnp.concatenate([l0, l0, l1, l0, l1, l2], 0)
            right = jnp.concatenate([r0, r1, r0, r2, r1, r0], 0)
            update = lax.dot_general(left, right, TN, preferred_element_type=jnp.float32)
            kept = jnp.where((wide_lane[:1] >= base) & (wide_lane[:1] < base + BLOCK), 0.0, 1.0)
            a_ref[first_row:, :] = a_ref[first_row:, :] * kept - update
            a_ref[pl.ds(pl.multiple_of(base, BLOCK), BLOCK), :] = panel
            return carry

        lax.fori_loop(0, LANES // BLOCK, step, 0)
    w_ref[...] = jnp.where(lane <= row, a_ref[...], 0.0) * lax.rsqrt(trace)

def inverse_factor(m, share):
    n = m.shape[0]
    return pl.pallas_call(
        functools.partial(factor_kernel, share),
        out_shape=jax.ShapeDtypeStruct((n, n), jnp.float32),
        in_specs=[pl.BlockSpec(memory_space=pltpu.VMEM)],
        out_specs=pl.BlockSpec(memory_space=pltpu.VMEM),
        scratch_shapes=[pltpu.VMEM((n, n), jnp.float32)],
        compiler_params=pltpu.CompilerParams(vmem_limit_bytes=VMEM_LIMIT),
        cost_estimate=pl.CostEstimate(flops=20_000_000, bytes_accessed=600_000, transcendentals=0),
    )(m)


def stacked_splits(row):
    n = row.shape[1]
    high = row.astype(jnp.bfloat16).astype(jnp.float32)
    rest = row - high
    mid = rest.astype(jnp.bfloat16).astype(jnp.float32)
    low = rest - mid
    at = lax.broadcasted_iota(jnp.int32, (8, n), 0)
    full = jnp.where(at == 0, high, jnp.where(at == 1, mid, jnp.where(at == 2, low, 0.0)))
    return full.astype(jnp.bfloat16)


def row_dot(stack, matrices, dims):
    total = None
    for matrix in matrices:
        part = lax.dot_general(stack, matrix, dims, preferred_element_type=jnp.float32)
        total = part if total is None else total + part
    return jnp.sum(total, axis=0, keepdims=True)


def put_scalars(values):
    at = lax.broadcasted_iota(jnp.int32, (1, LANES), 1)
    row = jnp.zeros((1, LANES), jnp.float32)
    for index, value in enumerate(values):
        row = jnp.where(at == index, value, row)
    return row


def total(row):
    return jnp.sum(row, axis=1, keepdims=True)


def forward_kernel(samples, first, *refs):
    if first:
        (grad_ref, q_ref, scale_ref, design_ref, s0_ref, s1_ref, inv_ref, vec_out, small_out, msg_out) = refs
        r = grad_ref[...]
        x = jnp.zeros_like(r)
        q = q_ref[...]
    else:
        (at_ref, msg_ref, vec_ref, small_ref, scales_ref, scale_ref, design_ref, s0_ref, s1_ref, inv_ref, vec_out, small_out, msg_out) = refs
        groups, n_col = msg_ref.shape[0], msg_ref.shape[1]
        feats = scale_ref.shape[1]
        width = inv_ref.shape[1]
        here = at_ref[0]
        squares = jnp.zeros((1, feats), jnp.float32)
        tail = jnp.zeros((1, width + LANES), jnp.float32)
        for col in range(n_col):
            back = msg_ref[0, col, :, :feats]
            tail = tail + msg_ref[0, col, :, feats:]
            for group in range(1, groups):
                back = back + msg_ref[group, col, :, :feats]
                tail = tail + msg_ref[group, col, :, feats:]
            pulled = scales_ref[col] * back
            squares = squares + pulled * pulled
        back = msg_ref[0, here, :, :feats]
        for group in range(1, groups):
            back = back + msg_ref[group, here, :, :feats]
        x, r, p = vec_ref[0:1], vec_ref[1:2], vec_ref[2:3]
        q, sp = small_ref[0:1], small_ref[1:2]
        agreement, length = small_ref[2:3, 0:1], small_ref[2:3, 1:2]
        bending = tail[:, width : width + 1] / (n_col * samples)
        curvature = bending + damping * length
        step = agreement / curvature
        product = scale_ref[...] * back / samples + damping * p
        x = x + step * p
        r = r - step * product
        pressed = tail[:, :width] / samples + damping * sp
        q = q - step * pressed
    inv = split(inv_ref[...], 3)
    s = row_dot(stacked_splits(q), inv, NN)
    s0, s1 = s0_ref[...], s1_ref[...]
    z = (r - row_dot(stacked_splits(s), (s0, s1), NN)) / damping
    if first:
        p, sp = z, samples * s
    else:
        solved = row_dot(stacked_splits(pressed), inv, NN)
        norm = total(squares) / (samples * samples) + 2.0 * damping * bending + damping * damping * length
        bent = (norm - total(pressed * solved)) / damping
        beta = step * step * bent / agreement - 1.0
        p, sp = z + beta * p, samples * s + beta * sp
    rounded = (scale_ref[...] * p).astype(jnp.bfloat16)
    ahead = lax.dot_general(
        jnp.broadcast_to(rounded, (8, rounded.shape[1])), design_ref[...], NT,
        preferred_element_type=jnp.float32,
    )[0:1]
    scalars = put_scalars((total(r * z), total(p * p)))
    message = jnp.concatenate([ahead, scalars], axis=1)
    for col in range(msg_out.shape[0]):
        msg_out[col] = message
    vec_out[...] = jnp.zeros_like(vec_out)
    vec_out[0:1] = x
    vec_out[1:2] = r
    vec_out[2:3] = p
    small_out[...] = jnp.zeros_like(small_out)
    small_out[0:1] = q
    small_out[1:2] = sp


def last_kernel(samples, msg_ref, vec_ref, weights_ref, x_out):
    rows = weights_ref.shape[2]
    bend = jnp.zeros((1, rows), jnp.float32)
    for group in range(msg_ref.shape[0]):
        y = msg_ref[group, 0, :, :rows]
        for col in range(1, msg_ref.shape[1]):
            y = y + msg_ref[group, col, :, :rows]
        inner = (weights_ref[group] * y).astype(jnp.bfloat16).astype(jnp.float32)
        bend = bend + inner * y
    tail = msg_ref[0, 0, :, rows:]
    for col in range(1, msg_ref.shape[1]):
        tail = tail + msg_ref[0, col, :, rows:]
    at = tail.shape[1] - LANES
    agreement, length = tail[:, at : at + 1], tail[:, at + 1 : at + 2]
    curvature = total(bend) / samples + damping * length
    x_out[...] = vec_ref[0:1] + agreement / curvature * vec_ref[2:3]


def backward_kernel(*refs):
    (msg_ref, small_ref, weight_ref, scale_ref, design_ref, s0_ref, s1_ref, small_out, msg_out) = refs
    rows = weight_ref.shape[1]
    width = small_ref.shape[1]
    sums = msg_ref[0]
    for col in range(1, msg_ref.shape[0]):
        sums = sums + msg_ref[col]
    y = sums[:, :rows]
    rest = sums[:, rows:]
    inner = (weight_ref[...] * y).astype(jnp.bfloat16)
    bend = total(inner.astype(jnp.float32) * y)
    at = lax.broadcasted_iota(jnp.int32, (1, width), 1)
    small_out[...] = jnp.zeros_like(small_out)
    small_out[0:2] = small_ref[0:2]
    small_out[2:3] = jnp.where(at == 0, rest[:, 0:1], jnp.where(at == 1, rest[:, 1:2], 0.0))
    back = lax.dot_general(
        jnp.broadcast_to(inner, (8, rows)), design_ref[...], NN, preferred_element_type=jnp.float32
    )[0:1]
    sb = row_dot(stacked_splits(scale_ref[...] * back), (s0_ref[...], s1_ref[...]), NT)
    message = jnp.concatenate([back, sb, put_scalars((bend,))], axis=1)
    for group in range(msg_out.shape[0]):
        for col in range(msg_out.shape[1]):
            msg_out[group, col] = message


def call(kernel, shapes, args, smem=0, flops=4_000_000):
    specs = [pl.BlockSpec(memory_space=pltpu.SMEM)] * smem
    specs += [pl.BlockSpec(memory_space=pltpu.VMEM)] * (len(args) - smem)
    return pl.pallas_call(
        kernel,
        out_shape=[jax.ShapeDtypeStruct(shape, jnp.float32) for shape in shapes],
        in_specs=specs,
        out_specs=[pl.BlockSpec(memory_space=pltpu.VMEM)] * len(shapes),
        compiler_params=pltpu.CompilerParams(vmem_limit_bytes=VMEM_LIMIT),
        cost_estimate=pl.CostEstimate(flops=flops, bytes_accessed=1_000_000, transcendentals=0),
    )(*args)


def heard_cols(row):
    n_col = lax.axis_size("cols")
    return lax.all_to_all(jnp.broadcast_to(row[None], (n_col, *row.shape)), "cols", 0, 0)


def summed_cols(row):
    return jnp.sum(heard_cols(row), 0)


def solve(design, weight, weights, feature_scale, scales, gradient, sketch, q, inverse, samples):
    n_row, n_col = lax.axis_size("rows"), lax.axis_size("cols")
    rows, feats = design.shape
    width = sketch.shape[0]
    scale = feature_scale[None]
    high = lax.reduce_precision(sketch, 8, 7)
    s0, s1 = high.astype(jnp.bfloat16), (sketch - high).astype(jnp.bfloat16)
    weight = weight[None]
    here = lax.axis_index("cols").astype(jnp.int32)[None]
    vec_shape, small_shape = (8, feats), (8, width)
    ahead_shape = (n_col, 1, rows + LANES)
    last_shape = (n_row * n_col, 1, rows + LANES)
    back_shape = (n_row, n_col, 1, feats + width + LANES)
    vec, small, message = call(
        functools.partial(forward_kernel, samples, True),
        (vec_shape, small_shape, ahead_shape),
        (gradient[None], q, scale, design, s0, s1, inverse),
    )
    for turn in range(1, ITERS):
        message = lax.all_to_all(message, "cols", 0, 0)
        small, message = call(
            backward_kernel,
            (small_shape, back_shape),
            (message, small, weight, scale, design, s0, s1),
        )
        message = message.reshape(n_row * n_col, 1, -1)
        message = lax.all_to_all(message, ("rows", "cols"), 0, 0).reshape(back_shape)
        vec, small, message = call(
            functools.partial(forward_kernel, samples, False),
            (vec_shape, small_shape, last_shape if turn + 1 == ITERS else ahead_shape),
            (here, message, vec, small, scales, scale, design, s0, s1, inverse),
            smem=1,
        )
    message = lax.all_to_all(message, ("rows", "cols"), 0, 0)
    (x,) = call(
        functools.partial(last_kernel, samples),
        ((1, feats),),
        (message.reshape(n_row, n_col, 1, -1), vec, weights),
    )
    return x[0]


def on_device(design, theta, feature_scale, labels, psi, phi):
    row_devices = lax.axis_size("rows")
    samples = design.shape[0] * row_devices
    width = psi.shape[1]
    scaled_theta = (theta * feature_scale).astype(jnp.bfloat16)
    part = jnp.dot(design, scaled_theta, preferred_element_type=jnp.float32)
    rows = part.shape[0]
    heard = heard_cols(jnp.concatenate([part, feature_scale])[None])
    margins = jnp.sum(heard[:, 0, :rows], 0)
    scales = heard[:, :, rows:]
    chance = jax.nn.sigmoid(margins)
    weight = chance * (1.0 - chance)
    misfit = (chance - labels.astype(jnp.float32)).astype(jnp.bfloat16)
    grad_part = jnp.dot(misfit, design, preferred_element_type=jnp.float32)
    rows_scaled = (
        design.astype(jnp.float32) * jnp.sqrt(weight)[:, None] * feature_scale[None, :]
    ).astype(jnp.bfloat16)
    mixed_cols = jnp.einsum(
        "rf,rs->fs", rows_scaled, psi, preferred_element_type=jnp.float32
    ).astype(jnp.bfloat16)
    range_rows = summed_blocks(
        jnp.dot(rows_scaled, mixed_cols, preferred_element_type=jnp.float32)
    )
    leaf_weights = shrink_weights(range_rows).astype(jnp.bfloat16)
    sketch = jnp.dot(leaf_weights, rows_scaled, preferred_element_type=jnp.float32)
    position = lax.axis_index("rows")

    def gradient_of(grad_sum):
        return feature_scale * grad_sum / samples + damping * theta

    for level in range(row_devices.bit_length() - 1):
        if level == 0:
            stacked, first, second, cross, grad_sum = leaf_gram(sketch, grad_part, position)
        else:
            stacked, first, second, cross, grad_sum, felt, weights_heard = merge_gram(
                sketch, gram, grad_sum, gradient_of, weight, position, level
            )
        full = jnp.concatenate(
            [jnp.concatenate([first, cross], 1), jnp.concatenate([cross.T, second], 1)], 0
        )
        weights = shrink_weights(jnp.dot(full, phi, precision=highest))
        sketch = jnp.dot(weights, stacked, precision=lax.Precision.HIGH)
        gram = lax.dot_general(
            jnp.dot(weights, full, precision=lax.Precision.HIGH), weights, NT, precision=lax.Precision.HIGH
        )
    q = lax.dot_general(felt, weights, NT, precision=lax.Precision.HIGH)
    kernel = gram + damping * samples * jnp.eye(width, dtype=jnp.float32)
    factor = inverse_factor(kernel, 0.0)
    inverse = jnp.dot(factor.T, factor, precision=highest)
    newton = solve(design, weight, weights_heard, feature_scale, scales, gradient_of(grad_sum), sketch, q, inverse, samples)
    return (newton, sketch)


def solution(mesh):
    in_specs = (P("rows", "cols"), P("cols"), P("cols"), P("rows"), P(), P())
    out_specs = (P("cols"), P(None, "cols"))
    return jax.shard_map(
        on_device, mesh=mesh, in_specs=in_specs, out_specs=out_specs, check_vma=False
    )
```
